32 devices in a mesh: band: 8 (over z, core), grid: 4 (over y, x).
Axes of the slice: x: 2, y: 2, z: 4, core: 2. Of those that a mesh axis runs over, the one named last changes fastest.
Arguments:
- orbitals: float32 [8, 48, 2304], P('band', 'grid'), may hold values from -6 to 6
Outputs:
- compressed: float32 [8, 48, 2304], P('band', 'grid')
The draws below stay inside these ranges and needn't reach their ends.
All inputs are finite; a program needn't handle non-finite values.
Results may differ from the reference program's by a relative error of at most 0.000092.
Values sent between devices are 32-bit elements; how exact they have to be, the bound alone decides.
A program may use at most 64 MiB of HBM per device.

```python
import jax
import jax.numpy as jnp
from jax import lax

NG = 48
BANDS = 8


def shard_levels(own_key, shape, pieces, least, top_value):
    level = 1.0
    for dim, blocks in pieces:
        steps = jax.random.uniform(jax.random.fold_in(jax.random.fold_in(own_key, 6), dim), (blocks,), jnp.float32, least / len(pieces), top_value / len(pieces))
        level = level * jnp.repeat(jnp.exp(steps), shape[dim] // blocks).reshape((-1,) + (1,) * (len(shape) - 1 - dim))
    return level


def centred(stream_key, shape, scale, limit, pieces=(), held_as=jnp.bfloat16):
    array = jax.random.normal(stream_key, shape, jnp.float32) * scale
    if len(pieces) > 0:
        array = shard_levels(stream_key, shape, pieces, -0.22, 0.18) * array
    return jnp.clip(array, min=-limit, max=limit).astype(held_as)


def setup_inputs(seed: int = 0) -> dict:
    seeds = jax.random.split(jax.random.key(seed), 2)
    orbitals = centred(seeds[0], (BANDS, NG, NG * NG), 1.0, 6.0, ((0, 8), (1, 4)), jnp.float32)
    return {"orbitals": orbitals}


coulomb_scale = 50.0

def coulomb_table(length):
    counter = jnp.arange(length, dtype=jnp.int32)
    signed = jnp.where(counter < length // 2, counter, counter - length).astype(jnp.float32)
    squares = signed * signed
    summed = squares[:, None, None] + squares[None, :, None] + squares[None, None, :]
    return jnp.where(summed > 0.0, coulomb_scale / jnp.maximum(summed, 1.0), 0.0)

def reference(orbitals):
    band_count = orbitals.shape[0]
    length = orbitals.shape[1]
    fields = orbitals.reshape(band_count, length, length, length)
    kernel = coulomb_table(length)

    def apply_one(orbital):
        density = orbital[None] * fields
        spectrum = jnp.fft.fftn(density, axes=(1, 2, 3))
        potential = jnp.real(jnp.fft.ifftn(spectrum * kernel, axes=(1, 2, 3)))
        return -jnp.sum(fields * potential, axis=0)
    exchange = lax.map(apply_one, fields)
    flat_orbitals = fields.reshape(band_count, -1)
    flat_exchange = exchange.reshape(band_count, -1)
    cells_total = float(length ** 3)
    projected = jnp.dot(flat_orbitals.astype(jnp.float32), flat_exchange.T.astype(jnp.float32), precision=lax.Precision.HIGHEST, preferred_element_type=jnp.float32) / cells_total
    definite = -0.5 * (projected + projected.T)
    lower = jnp.linalg.cholesky(definite)
    inverse_lower = jax.scipy.linalg.solve_triangular(lower, jnp.eye(band_count, dtype=jnp.float32), lower=True)
    compressed = jnp.dot(inverse_lower.astype(jnp.float32), flat_exchange.astype(jnp.float32), precision=lax.Precision.HIGHEST, preferred_element_type=jnp.float32)
    return compressed.reshape(orbitals.shape)
```

```python
import functools
import math

import jax
import jax.numpy as jnp
import numpy as np
from jax import lax
from jax.experimental import pallas as pl
from jax.experimental.pallas import tpu as pltpu
from jax.sharding import PartitionSpec as P

MESH = pl.DeviceIdType.MESH
F32 = jnp.float32
BF16 = jnp.bfloat16
coulomb_scale = 50.0


def real_basis(length):
    n = np.arange(length)[:, None]
    m = np.arange(length)[None, :]
    angle = 2.0 * math.pi * ((n * np.minimum(m, length - m)) % length) / length
    table = np.where(m <= length // 2, np.cos(angle), np.sin(angle))
    weight = np.where((m == 0) | (2 * m == length), 1.0, 2.0)
    return table * np.sqrt(weight / length)


def split(value):
    high = value.astype(BF16)
    return high, (value - high.astype(F32)).astype(BF16)


def right(value, table):
    both = jnp.concatenate(split(value), axis=1)
    out = jnp.dot(both, table, preferred_element_type=F32)
    half = out.shape[1] // 2
    return out[:, :half] + out[:, half:]


def left(table, value):
    both = jnp.concatenate(split(value), axis=0)
    out = jnp.dot(table, both, preferred_element_type=F32)
    half = out.shape[0] // 2
    return out[:half] + out[half:]


def kernel(
    bands, grids, length, pieces,
    phi, wide, tall, out,
    slabs, own, part, field, sums, exs, proj_grid, proj_band,
    dense_own, dense_part, work, coulomb, dense_field,
    sem_local, slab_send, slab_recv, fwd_send,
    own_send, own_recv, part_send, part_recv, pfwd_send, pfwd_recv,
    sum_send, sum_recv, ex_send, ex_recv, xfwd_send,
    pg_send, pg_recv, pb_send, pb_recv,
):
    b = lax.axis_index("band")
    g = lax.axis_index("grid")
    p = b // 2
    c = b % 2
    sibling = p * 2 + (1 - c)
    rows = length // grids
    pairs = bands // 2
    step = 8
    chunk = step * length
    chunks = length // step
    width = length * length // pieces
    per_piece = chunks // pieces

    def remote(src, dst, send, recv, band, grid):
        return pltpu.make_async_remote_copy(
            src_ref=src, dst_ref=dst, send_sem=send, recv_sem=recv,
            device_id=(band, grid), device_id_type=MESH,
        )

    def cut(q):
        return pl.ds(q * width, width)

    local = pltpu.make_async_copy(phi, slabs.at[b], sem_local)
    local.start()

    barrier = pltpu.get_barrier_semaphore()
    for off in range(1, bands):
        pl.semaphore_signal(barrier, inc=1, device_id=(lax.rem(b + off, bands), g), device_id_type=MESH)
    for off in range(1, grids):
        pl.semaphore_signal(barrier, inc=1, device_id=(b, lax.rem(g + off, grids)), device_id_type=MESH)

    def freq_of(m):
        f = jnp.minimum(m, length - m).astype(F32)
        return f * f

    def freq(shape, dim, base):
        return freq_of(lax.broadcasted_iota(jnp.int32, shape, dim) + base)

    def coulomb_step(i, carry):
        shape = (step, length, 128)
        lane = lax.broadcasted_iota(jnp.int32, shape, 2)
        lane = jnp.where(lane < length, lane, lane - length)
        squared = freq(shape, 0, i * step) + freq(shape, 1, 0) + freq_of(lane)
        coulomb[pl.ds(i * step, step)] = jnp.where(
            squared > 0.0, coulomb_scale / jnp.maximum(squared, 1.0), 0.0
        )
        return carry

    with jax.named_scope("coul"):
        lax.fori_loop(0, chunks, coulomb_step, 0)
        local.wait()
    with jax.named_scope("barr"):
        pl.semaphore_wait(barrier, bands + grids - 2)

    waits = []

    def go(copy):
        copy.start()
        waits.append(copy)

    for q in range(pieces):
        for off in range(1, pairs):
            peer = lax.rem(p + off, pairs) * 2 + c
            go(remote(phi.at[:, cut(q)], slabs.at[b, :, cut(q)],
                      slab_send.at[off, q], slab_recv.at[b, q], peer, g))
        for off in range(1, grids):
            go(remote(phi.at[:, cut(q)], own.at[g, :, cut(q)],
                      own_send.at[off, q], own_recv.at[g, q], b, lax.rem(g + off, grids)))
        go(remote(phi.at[:, cut(q)], slabs.at[b, :, cut(q)],
                  slab_send.at[0, q], slab_recv.at[b, q], sibling, g))

    def partner_copy(pair, q):
        return remote(
            slabs.at[pair * 2 + c, :, cut(q)], part.at[c, g, :, cut(q)],
            part_send.at[pair, q], part_recv.at[g, q], b, pair,
        )

    def to_partner(pair, q):
        @pl.when(pair != g)
        def _():
            partner_copy(pair, q).start()

    def slab_arrival(band, q):
        here = slabs.at[band, :, cut(q)]
        remote(here, here, slab_send.at[0, q], slab_recv.at[band, q], sibling, g).wait_recv()

    def pass_slabs(q):
        to_partner(p, q)
        for off in range(1, pairs):
            pair = lax.rem(p + off, pairs)
            band = pair * 2 + c
            slab_arrival(band, q)
            to_partner(pair, q)
            here = slabs.at[band, :, cut(q)]
            go(remote(here, here, fwd_send.at[off, q], slab_recv.at[band, q], sibling, g))

    def pass_partners(q):
        for off in range(1, grids):
            other = lax.rem(g + off, grids)
            here = part.at[c, other, :, cut(q)]
            remote(here, here, part_send.at[0, q], part_recv.at[other, q], b, other).wait_recv()
            go(remote(here, here, pfwd_send.at[off, q], pfwd_recv.at[other, q], sibling, g))

    def collect(q):
        slab_arrival(2 * g + 1 - c, q)
        for off in range(1, grids):
            other = lax.rem(g + off, grids)
            here = own.at[other, :, cut(q)]
            remote(here, here, own_send.at[0, q], own_recv.at[other, q], b, other).wait_recv()
            here = part.at[1 - c, other, :, cut(q)]
            remote(here, here, part_send.at[0, q], pfwd_recv.at[other, q], sibling, g).wait_recv()
        own[g, :, cut(q)] = phi[:, cut(q)]
        for k in range(2):
            part[k, g, :, cut(q)] = slabs[2 * g + k, :, cut(q)]
        for s in range(grids):
            here = slice(s * rows, (s + 1) * rows)
            dense_own[here, cut(q)] = own[s, :, cut(q)]
            for k in range(2):
                dense_part[k, here, cut(q)] = part[k, s, :, cut(q)]

    padding = jnp.zeros((128 - 2 * length, chunk), F32)

    def rows_of(m):
        return pl.ds(pl.multiple_of(m * length, 8), length)

    def lanes_of(i):
        return pl.ds(pl.multiple_of(i * chunk, 128), chunk)

    def stage_in(i, carry):
        lanes = lanes_of(i)
        mine = dense_own[:, lanes]
        density = [mine * dense_part[k, :, lanes] for k in range(2)]
        value = right(jnp.concatenate(density + [padding], axis=0).T, wide[0])
        for s in range(0, step, 2):
            two = jnp.concatenate([value[n * length:(n + 1) * length] for n in (s, s + 1)], axis=1)
            two = left(tall[0], two)
            for n in range(2):
                work[rows_of(i * step + s + n), :] = two[:, n * 128:(n + 1) * 128]
        return carry

    def stage_mid(i, carry):
        for s in range(0, step, 2):
            here = [pl.ds(i * step + s + n, length, length) for n in range(2)]
            two = left(tall[0], jnp.concatenate([work[h, :] for h in here], axis=1))
            two = two * jnp.concatenate([coulomb[i * step + s + n] for n in range(2)], axis=1)
            two = left(tall[1], two)
            for n in range(2):
                work[here[n], :] = two[:, n * 128:(n + 1) * 128]
        return carry

    def send_sums(i):
        lanes = lanes_of(i)
        for off in range(1, grids):
            other = lax.rem(g + off, grids)
            remote(field.at[other, :, lanes], sums.at[g, :, lanes],
                   sum_send.at[off, i], sum_recv.at[g, i], b, other).start()

    def stage_out(i, carry):
        lanes = lanes_of(i)
        value = []
        for s in range(0, step, 2):
            two = jnp.concatenate([work[rows_of(i * step + s + n), :] for n in range(2)], axis=1)
            two = left(tall[1], two)
            value += [two[:, n * 128:(n + 1) * 128] for n in range(2)]
        value = right(jnp.concatenate(value, axis=0), wide[1]).T
        dense_field[...] = sum(
            dense_part[k, :, lanes] * value[k * length:(k + 1) * length] for k in range(2)
        )
        for s in range(grids):
            field[s, :, lanes] = dense_field[s * rows:(s + 1) * rows, :]

        @pl.when(i > 0)
        def _():
            send_sums(i - 1)

        return carry

    columns = [None] * bands

    def exchange_piece(q):
        for i in range(q * per_piece, (q + 1) * per_piece):
            lanes = pl.ds(i * chunk, chunk)
            for off in range(1, grids):
                other = lax.rem(g + off, grids)
                here = sums.at[other, :, lanes]
                remote(here, here, sum_send.at[0, i], sum_recv.at[other, i], b, other).wait_recv()
        value = field[g, :, cut(q)]
        for off in range(1, grids):
            value = value + sums[lax.rem(g + off, grids), :, cut(q)]
        value = -value
        exs[b, :, cut(q)] = value
        for k in range(bands):
            product = jnp.sum(slabs[k, :, cut(q)] * value, axis=0, keepdims=True)
            product = sum(product[:, n:n + 128] for n in range(0, width, 128))
            columns[k] = product if columns[k] is None else columns[k] + product
        here = exs.at[b, :, cut(q)]
        for off in range(1, pairs):
            peer = lax.rem(p + off, pairs) * 2 + c
            go(remote(here, here, ex_send.at[off, q], ex_recv.at[b, q], peer, g))
        go(remote(here, here, ex_send.at[0, q], ex_recv.at[b, q], sibling, g))

    for q in range(pieces):
        with jax.named_scope(f"pslab{q}"):
            pass_slabs(q)
        if q >= 1:
            with jax.named_scope(f"ppart{q-1}"):
                pass_partners(q - 1)
    for q in range(pieces):
        with jax.named_scope(f"collect{q}"):
            collect(q)
        with jax.named_scope(f"stagein{q}"):
            lax.fori_loop(q * per_piece, (q + 1) * per_piece, stage_in, 0, unroll=2)
        if q == 0:
            with jax.named_scope("ppartlast"):
                pass_partners(pieces - 1)
    with jax.named_scope("mid"):
        lax.fori_loop(0, chunks, stage_mid, 0, unroll=6)
    for q in range(pieces):
        for off in range(pairs):
            pair = lax.rem(p + off, pairs)

            @pl.when(pair != g)
            def _(pair=pair, q=q):
                slab_arrival(pair * 2 + 1 - c, q)

    with jax.named_scope("out"):
        for q in range(pieces):
            lax.fori_loop(q * per_piece, (q + 1) * per_piece, stage_out, 0, unroll=2)
        send_sums(chunks - 1)
    for q in range(pieces):
        with jax.named_scope(f"exch{q}"):
            exchange_piece(q)

    total = jnp.sum(jnp.concatenate(columns, axis=0), axis=1, keepdims=True)
    proj_grid[g] = jnp.broadcast_to(total, (bands, 128))
    for off in range(1, grids):
        other = lax.rem(g + off, grids)
        go(remote(proj_grid.at[g], proj_grid.at[g], pg_send.at[off], pg_recv.at[g], b, other))

    def ex_arrival(band, q):
        here = exs.at[band, :, cut(q)]
        remote(here, here, ex_send.at[0, q], ex_recv.at[band, q], sibling, g).wait_recv()

    def pass_exchange(q):
        for off in range(1, pairs):
            band = lax.rem(p + off, pairs) * 2 + c
            ex_arrival(band, q)
            here = exs.at[band, :, cut(q)]
            go(remote(here, here, xfwd_send.at[off, q], ex_recv.at[band, q], sibling, g))

    pass_exchange(0)
    for off in range(1, grids):
        other = lax.rem(g + off, grids)
        here = proj_grid.at[other]
        remote(here, here, pg_send.at[0], pg_recv.at[other], b, other).wait_recv()
    total = proj_grid[0]
    for s in range(1, grids):
        total = total + proj_grid[s]
    proj_band[b] = total
    for off in range(1, bands):
        other = lax.rem(b + off, bands)
        go(remote(proj_band.at[b], proj_band.at[b], pb_send.at[off], pb_recv.at[b], other, g))
    for q in range(1, pieces):
        pass_exchange(q)
    for off in range(1, bands):
        other = lax.rem(b + off, bands)
        here = proj_band.at[other]
        remote(here, here, pb_send.at[0], pb_recv.at[other], other, g).wait_recv()

    row = lax.broadcasted_iota(jnp.int32, (bands, 128), 0)
    col = lax.broadcasted_iota(jnp.int32, (bands, 128), 1)
    matrix = jnp.zeros((bands, 128), F32)
    mirrored = jnp.zeros((bands, 128), F32)
    for l in range(bands):
        entries = proj_band[l]
        matrix = jnp.where(col == l, entries, matrix)
        flipped = jnp.sum(jnp.where(row == col, entries, 0.0), axis=0, keepdims=True)
        mirrored = jnp.where(row == l, flipped, mirrored)
    definite = (matrix + mirrored) * (-0.5 / float(length**3))
    definite = jnp.where(col < bands, definite, jnp.where(col == row + bands, 1.0, 0.0))
    for j in range(bands - 1):
        line = definite[j:j + 1, :]
        ratio = definite[:, j:j + 1] / definite[j:j + 1, j:j + 1]
        definite = definite - jnp.where(row > j, ratio * line, 0.0)
    pick = jnp.sum(jnp.where(row == b, definite, 0.0), axis=0, keepdims=True)
    pivot = jnp.sum(jnp.where(col[0:1] == b, pick, 0.0), axis=1, keepdims=True)
    pick = pick / jnp.sqrt(pivot)

    for q in range(pieces):
        for off in range(pairs):
            ex_arrival(lax.rem(p + off, pairs) * 2 + (1 - c), q)
    result = jnp.zeros(phi.shape, F32)
    for l in range(bands):
        result = result + pick[:, bands + l:bands + l + 1] * exs[l]
    out[...] = result

    for copy in waits:
        copy.wait_send()
    for i in range(chunks):
        lanes = pl.ds(i * chunk, chunk)
        for off in range(1, grids):
            other = lax.rem(g + off, grids)
            remote(field.at[other, :, lanes], sums.at[g, :, lanes],
                   sum_send.at[off, i], sum_recv.at[g, i], b, other).wait_send()
    for q in range(pieces):
        for off in range(pairs):
            pair = lax.rem(p + off, pairs)

            @pl.when(pair != g)
            def _(pair=pair, q=q):
                partner_copy(pair, q).wait_send()


def per_device(bands, grids, orbitals):
    blocks, rows, cells = orbitals.shape
    length = rows * grids
    assert blocks == 1 and bands == 2 * grids and length * length == cells
    assert 2 * length <= 128
    basis = real_basis(length)
    wide, tall = [], []
    for table in (basis, basis.T):
        high = table.astype(np.float32).astype(BF16).astype(np.float64)
        both = []
        for part in (high, table - high):
            block = np.zeros((128, 128))
            for k in range(2):
                here = slice(k * length, (k + 1) * length)
                block[here, here] = part
            both.append(block)
        wide.append(np.tile(np.concatenate(both, axis=1), (2, 1)))
        tall.append(np.tile(np.concatenate([high.T, (table - high).T], axis=0), (1, 2)))
    wide = jnp.asarray(np.stack(wide).astype(BF16))
    tall = jnp.asarray(np.stack(tall).astype(BF16))
    slab = (rows, cells)
    dma = lambda *n: pltpu.SemaphoreType.DMA(n)
    vmem = lambda *shape: pltpu.VMEM(shape, F32)
    pairs = bands // 2
    pieces = 3
    chunks = length // 8
    result = pl.pallas_call(
        functools.partial(kernel, bands, grids, length, pieces),
        out_shape=jax.ShapeDtypeStruct(slab, F32),
        in_specs=[pl.BlockSpec(memory_space=pltpu.VMEM)] * 3,
        out_specs=pl.BlockSpec(memory_space=pltpu.VMEM),
        scratch_shapes=[
            vmem(bands, *slab), vmem(grids, *slab), vmem(2, grids, *slab),
            vmem(grids, *slab), vmem(grids, *slab), vmem(bands, *slab),
            vmem(grids, bands, 128), vmem(bands, bands, 128),
            vmem(length, cells), vmem(2, length, cells),
            vmem(length * length, 128), vmem(length, length, 128),
            vmem(length, 8 * length),
            pltpu.SemaphoreType.DMA,
            dma(pairs, pieces), dma(bands, pieces), dma(pairs, pieces),
            dma(grids, pieces), dma(grids, pieces), dma(pairs, pieces), dma(grids, pieces),
            dma(grids, pieces), dma(grids, pieces),
            dma(grids, chunks), dma(grids, chunks),
            dma(pairs, pieces), dma(bands, pieces), dma(pairs, pieces),
            dma(grids), dma(grids), dma(bands), dma(bands),
        ],
        compiler_params=pltpu.CompilerParams(
            collective_id=0, has_side_effects=True, vmem_limit_bytes=40 * 1024 * 1024
        ),
    )(orbitals.reshape(slab), wide, tall)
    return result.reshape(orbitals.shape)


def solution(mesh):
    bands, grids = mesh.shape["band"], mesh.shape["grid"]
    return jax.shard_map(
        functools.partial(per_device, bands, grids), mesh=mesh,
        in_specs=(P("band", "grid", None),), out_specs=P("band", "grid", None), check_vma=False,
    )
```

```python
import functools
import math

import jax
import jax.numpy as jnp
import numpy as np
from jax import lax
from jax.experimental import pallas as pl
from jax.experimental.pallas import tpu as pltpu
from jax.sharding import PartitionSpec as P

MESH = pl.DeviceIdType.MESH
F32 = jnp.float32
BF16 = jnp.bfloat16
coulomb_scale = 50.0
reach = 2


def real_basis(length):
    n = np.arange(length)[:, None]
    m = np.arange(length)[None, :]
    angle = 2.0 * math.pi * ((n * np.minimum(m, length - m)) % length) / length
    table = np.where(m <= length // 2, np.cos(angle), np.sin(angle))
    weight = np.where((m == 0) | (2 * m == length), 1.0, 2.0)
    return table * np.sqrt(weight / length)


def split(value):
    high = value.astype(BF16)
    return high, (value - high.astype(F32)).astype(BF16)


def right(value, table):
    both = jnp.concatenate(split(value), axis=1)
    out = jnp.dot(both, table, preferred_element_type=F32)
    half = out.shape[1] // 2
    return out[:, :half] + out[:, half:]


def left(table, value):
    both = jnp.concatenate(split(value), axis=0)
    out = jnp.dot(table, both, preferred_element_type=F32)
    half = out.shape[0] // 2
    return out[:half] + out[half:]


def kernel(
    bands, grids, length, pieces,
    phi, consts, out,
    slabs, cubes, field, sums, exs, proj_grid, proj_band,
    dense_own, dense_part, work, coulomb, dense_field, tables,
    phi_sem, own_sem, consts_sem, slab_send, slab_recv, relay_send, fwd_send, fwd_recv,
    own_send, own_recv, part_send, part_recv, pfwd_send, pfwd_recv,
    sum_send, sum_recv, ex_send, ex_recv, xrelay_send, xfwd_send,
    pg_send, pg_recv, pb_send, pb_recv,
):
    b = lax.axis_index("band")
    g = lax.axis_index("grid")
    p = b // 2
    c = b % 2
    sibling = p * 2 + (1 - c)
    rows = length // grids
    pairs = bands // 2
    step = 8
    chunk = step * length
    chunks = length // step
    width = length * length // pieces
    per_piece = chunks // pieces
    others = range(1, grids)

    def remote(src, dst, send, recv, band, grid):
        return pltpu.make_async_remote_copy(
            src_ref=src, dst_ref=dst, send_sem=send, recv_sem=recv,
            device_id=(band, grid), device_id_type=MESH,
        )

    def cut(q):
        return pl.ds(q * width, width)

    def on_line(layer):
        return (layer >= 0) & (layer < pairs)

    sent = []

    def go(make, when=None):
        if when is None:
            make().start()
        else:
            @pl.when(when)
            def _():
                make().start()
        sent.append((make, when))

    def peer(off):
        return lax.rem(g + off, grids)

    barrier = pltpu.get_barrier_semaphore()
    expected = 1 + grids - 1
    pl.semaphore_signal(barrier, inc=1, device_id=(sibling, g), device_id_type=MESH)
    for off in others:
        pl.semaphore_signal(barrier, inc=1, device_id=(b, peer(off)), device_id_type=MESH)
    for d in range(1, min(reach, pairs - 1) + 1):
        for sign in (1, -1):
            layer = p + sign * d

            @pl.when(on_line(layer))
            def _(layer=layer):
                pl.semaphore_signal(barrier, inc=1, device_id=(layer * 2 + c, g), device_id_type=MESH)

            expected = expected + on_line(layer).astype(jnp.int32)

    local = []
    for x in range(rows):
        local.append(pltpu.make_async_copy(phi.at[x], slabs.at[b, pl.ds(x, 1), :], phi_sem.at[x]))
    for x in range(rows):
        local.append(pltpu.make_async_copy(phi.at[x], cubes.at[0, g, pl.ds(x, 1), :], own_sem.at[x]))
    local.append(pltpu.make_async_copy(consts, tables, consts_sem))
    for copy in local:
        copy.start()

    def freq_of(m):
        f = jnp.minimum(m, length - m).astype(F32)
        return f * f

    def freq(shape, dim, base):
        return freq_of(lax.broadcasted_iota(jnp.int32, shape, dim) + base)

    def coulomb_step(i, carry):
        shape = (step, length, 128)
        lane = lax.broadcasted_iota(jnp.int32, shape, 2)
        lane = jnp.where(lane < length, lane, lane - length)
        squared = freq(shape, 0, i * step) + freq(shape, 1, 0) + freq_of(lane)
        coulomb[pl.ds(i * step, step)] = jnp.where(
            squared > 0.0, coulomb_scale / jnp.maximum(squared, 1.0), 0.0
        )
        return carry

    with jax.named_scope("coul"):
        lax.fori_loop(0, chunks, coulomb_step, 0)
        for copy in local:
            copy.wait()
    with jax.named_scope("barr"):
        pl.semaphore_wait(barrier, expected)

    def slab_copy(src_band, layer, q, send):
        here = slabs.at[src_band, :, cut(q)]
        return remote(here, here, send, slab_recv.at[src_band, q], layer * 2 + c, g)

    def sibling_part(s, q, src):
        return remote(src, cubes.at[1 + c, s, :, cut(q)], pfwd_send.at[s, q], pfwd_recv.at[s, q], sibling, g)

    for q in range(pieces):
        for d in range(min(reach, pairs - 1), 0, -1):
            for sign in (1, -1):
                layer = p + sign * d
                index = 2 * (d - 1) + (sign < 0)
                go(lambda layer=layer, index=index, q=q: slab_copy(b, layer, q, slab_send.at[index, q]),
                   on_line(layer))
        for off in others:
            go(lambda off=off, q=q: remote(
                slabs.at[b, :, cut(q)], cubes.at[0, g, :, cut(q)],
                own_send.at[off, q], own_recv.at[g, q], b, peer(off)))
        go(lambda q=q: sibling_part(g, q, slabs.at[b, :, cut(q)]), g == p)

    def partner_copy(layer, q):
        return remote(
            slabs.at[layer * 2 + c, :, cut(q)], cubes.at[1 + c, g, :, cut(q)],
            part_send.at[layer, q], part_recv.at[g, q], b, layer,
        )

    def take_slab(sign, d, q):
        layer = p - sign * d
        band = layer * 2 + c
        there = on_line(layer)

        @pl.when(there)
        def _():
            slab_copy(band, p, q, slab_send.at[0, q]).wait_recv()

        if d >= reach:
            way = 2 * d + (sign < 0)
            go(lambda: slab_copy(band, p + sign, q, relay_send.at[way, q]), there & on_line(p + sign))
        go(lambda: partner_copy(layer, q), there & (layer != g))
        go(lambda: sibling_part(g, q, slabs.at[band, :, cut(q)]), there & (layer == g))

    def take_part(off, q):
        other = peer(off)
        mine = cubes.at[0, other, :, cut(q)]
        remote(mine, mine, own_send.at[0, q], own_recv.at[other, q], b, other).wait_recv()
        slot = jnp.where(g == p, 0, 1 + c)

        @pl.when(g != p)
        def _():
            here = cubes.at[1 + c, other, :, cut(q)]
            remote(here, here, part_send.at[0, q], part_recv.at[other, q], b, other).wait_recv()

        go(lambda: sibling_part(other, q, cubes.at[slot, other, :, cut(q)]))

    def collect(q):
        for s in range(grids):
            here = cubes.at[2 - c, s, :, cut(q)]
            remote(here, here, pfwd_send.at[0, q], pfwd_recv.at[s, q], sibling, g).wait_recv()
        slot = jnp.where(g == p, 0, 1 + c)
        for s in range(grids):
            here = slice(s * rows, (s + 1) * rows)
            dense_own[here, cut(q)] = cubes[0, s, :, cut(q)]
            dense_part[1 - c, here, cut(q)] = cubes[2 - c, s, :, cut(q)]

            @pl.when(s != g)
            def _(s=s, here=here):
                dense_part[c, here, cut(q)] = cubes[slot, s, :, cut(q)]

            @pl.when(s == g)
            def _(s=s, here=here):
                dense_part[c, here, cut(q)] = slabs[2 * g + c, :, cut(q)]

    padding = jnp.zeros((128 - 2 * length, chunk), F32)

    def wide(n):
        return tables[n, 0:256, :]

    def tall(n):
        return tables[n, 256:256 + 2 * length, 0:2 * length]

    def rows_of(m):
        return pl.ds(pl.multiple_of(m * length, 8), length)

    def lanes_of(i):
        return pl.ds(pl.multiple_of(i * chunk, 128), chunk)

    def stage_in(i, carry):
        lanes = lanes_of(i)
        mine = dense_own[:, lanes]
        density = [mine * dense_part[k, :, lanes] for k in range(2)]
        value = right(jnp.concatenate(density + [padding], axis=0).T, wide(0))
        for s in range(0, step, 2):
            two = jnp.concatenate([value[n * length:(n + 1) * length] for n in (s, s + 1)], axis=1)
            two = left(tall(0), two)
            for n in range(2):
                work[rows_of(i * step + s + n), :] = two[:, n * 128:(n + 1) * 128]
        return carry

    def stage_mid(i, carry):
        for s in range(0, step, 2):
            here = [pl.ds(i * step + s + n, length, length) for n in range(2)]
            two = left(tall(0), jnp.concatenate([work[h, :] for h in here], axis=1))
            two = two * jnp.concatenate([coulomb[i * step + s + n] for n in range(2)], axis=1)
            two = left(tall(1), two)
            for n in range(2):
                work[here[n], :] = two[:, n * 128:(n + 1) * 128]
        return carry

    def sum_copy(i, off):
        lanes = lanes_of(i)
        other = peer(off)
        return remote(field.at[other, :, lanes], sums.at[g, :, lanes],
                      sum_send.at[off, i], sum_recv.at[g, i], b, other)

    def send_sums(i):
        for off in others:
            sum_copy(i, off).start()

    def stage_out(i, carry):
        lanes = lanes_of(i)
        value = []
        for s in range(0, step, 2):
            two = jnp.concatenate([work[rows_of(i * step + s + n), :] for n in range(2)], axis=1)
            two = left(tall(1), two)
            value += [two[:, n * 128:(n + 1) * 128] for n in range(2)]
        value = right(jnp.concatenate(value, axis=0), wide(1)).T
        dense_field[...] = sum(
            dense_part[k, :, lanes] * value[k * length:(k + 1) * length] for k in range(2)
        )
        for s in range(grids):
            field[s, :, lanes] = dense_field[s * rows:(s + 1) * rows, :]

        @pl.when(i > 0)
        def _():
            send_sums(i - 1)

        return carry

    columns = [None] * bands

    def ex_copy(src_band, band, q, send):
        here = exs.at[src_band, :, cut(q)]
        return remote(here, here, send, ex_recv.at[src_band, q], band, g)

    def exchange_piece(q):
        for i in range(q * per_piece, (q + 1) * per_piece):
            lanes = pl.ds(i * chunk, chunk)
            for off in others:
                other = peer(off)
                here = sums.at[other, :, lanes]
                remote(here, here, sum_send.at[0, i], sum_recv.at[other, i], b, other).wait_recv()
        value = field[g, :, cut(q)]
        for off in others:
            value = value + sums[peer(off), :, cut(q)]
        value = -value
        exs[b, :, cut(q)] = value
        for d in range(min(reach, pairs - 1), 0, -1):
            go(lambda d=d: ex_copy(b, (p + d) * 2 + c, q, ex_send.at[d, q]), on_line(p + d))
        go(lambda: ex_copy(b, sibling, q, ex_send.at[0, q]), c == 0)
        for k in range(bands):
            product = jnp.sum(slabs[k, :, cut(q)] * value, axis=0, keepdims=True)
            product = sum(product[:, n:n + 128] for n in range(0, width, 128))
            columns[k] = product if columns[k] is None else columns[k] + product

    near = range(1, min(reach, pairs - 1) + 1)
    far = range(reach + 1, pairs)
    with jax.named_scope("slabnear"):
        for q in range(pieces):
            for d in near:
                for sign in (1, -1):
                    take_slab(sign, d, q)
    with jax.named_scope("slabfar"):
        for d in far:
            for q in range(pieces):
                for sign in (1, -1):
                    take_slab(sign, d, q)
    for q in range(pieces):
        with jax.named_scope(f"part{q}"):
            for off in others:
                take_part(off, q)
        if q >= 1:
            with jax.named_scope(f"collect{q-1}"):
                collect(q - 1)
            with jax.named_scope(f"stagein{q-1}"):
                lax.fori_loop((q - 1) * per_piece, q * per_piece, stage_in, 0, unroll=True)
    with jax.named_scope("collectlast"):
        collect(pieces - 1)
    with jax.named_scope("stageinlast"):
        lax.fori_loop((pieces - 1) * per_piece, chunks, stage_in, 0, unroll=True)

    def whole_slab(band):
        here = slabs.at[band]
        return remote(here, here, fwd_send.at[band], fwd_recv.at[band], sibling, g)

    for s in range(pairs):
        go(lambda s=s: whole_slab(2 * s + c))
    with jax.named_scope("mid"):
        lax.fori_loop(0, chunks, stage_mid, 0, unroll=True)
    with jax.named_scope("out"):
        for q in range(pieces):
            lax.fori_loop(q * per_piece, (q + 1) * per_piece, stage_out, 0, unroll=True)
        send_sums(chunks - 1)
        for s in range(pairs):
            whole_slab(2 * s + 1 - c).wait_recv()
    for q in range(pieces):
        with jax.named_scope(f"exch{q}"):
            exchange_piece(q)

    total = jnp.sum(jnp.concatenate(columns, axis=0), axis=1, keepdims=True)
    proj_grid[g] = jnp.broadcast_to(total, (bands, 128))
    for off in others:
        go(lambda off=off: remote(proj_grid.at[g], proj_grid.at[g], pg_send.at[off], pg_recv.at[g], b, peer(off)))

    def take_exchange(d, q):
        layer = p - d
        band = layer * 2 + c
        there = layer >= 0

        @pl.when(there)
        def _():
            ex_copy(band, b, q, ex_send.at[0, q]).wait_recv()

        if d >= reach:
            go(lambda: ex_copy(band, (p + 1) * 2 + c, q, xrelay_send.at[d, q]), there & on_line(p + 1))
        go(lambda: ex_copy(band, sibling, q, xfwd_send.at[d, q]), there)

    with jax.named_scope("pex0"):
        for d in near:
            take_exchange(d, 0)
    with jax.named_scope("projgrid"):
        for off in others:
            other = peer(off)
            here = proj_grid.at[other]
            remote(here, here, pg_send.at[0], pg_recv.at[other], b, other).wait_recv()
        total = proj_grid[0]
        for s in range(1, grids):
            total = total + proj_grid[s]
        proj_band[b] = total
    for off in range(1, bands):
        go(lambda off=off: remote(
            proj_band.at[b], proj_band.at[b], pb_send.at[off], pb_recv.at[b], b + off, g), b + off < bands)
    with jax.named_scope("pexnear"):
        for q in range(1, pieces):
            for d in near:
                take_exchange(d, q)
    with jax.named_scope("pexfar"):
        for d in far:
            for q in range(pieces):
                take_exchange(d, q)
    with jax.named_scope("projband"):
        for l in range(bands - 1):
            @pl.when(l < b)
            def _(l=l):
                here = proj_band.at[l]
                remote(here, here, pb_send.at[0], pb_recv.at[l], l, g).wait_recv()

    row = lax.broadcasted_iota(jnp.int32, (bands, 128), 0)
    col = lax.broadcasted_iota(jnp.int32, (bands, 128), 1)
    matrix = jnp.zeros((bands, 128), F32)
    mirrored = jnp.zeros((bands, 128), F32)
    for l in range(bands):
        entries = proj_band[l]
        matrix = jnp.where(col == l, entries, matrix)
        flipped = jnp.sum(jnp.where(row == col, entries, 0.0), axis=0, keepdims=True)
        mirrored = jnp.where(row == l, flipped, mirrored)
    definite = (matrix + mirrored) * (-0.5 / float(length**3))
    unit = (col == row) | (col == row + bands)
    definite = jnp.where((row <= b) & (col <= b), definite, jnp.where(unit, 1.0, 0.0))
    for j in range(bands - 1):
        line = definite[j:j + 1, :]
        ratio = definite[:, j:j + 1] / definite[j:j + 1, j:j + 1]
        definite = definite - jnp.where(row > j, ratio * line, 0.0)
    pick = jnp.sum(jnp.where(row == b, definite, 0.0), axis=0, keepdims=True)
    pivot = jnp.sum(jnp.where(col[0:1] == b, pick, 0.0), axis=1, keepdims=True)
    pick = pick / jnp.sqrt(pivot)

    with jax.named_scope("final"):
        for q in range(pieces):
            for d in range(pairs):
                layer = p - d

                @pl.when((layer >= 0) if d > 0 else (c == 1))
                def _(layer=layer):
                    ex_copy(layer * 2 + 1 - c, b, q, ex_send.at[0, q]).wait_recv()

            result = jnp.zeros((rows, width), F32)
            for l in range(bands):
                result = result + pick[:, bands + l:bands + l + 1] * jnp.where(l <= b, exs[l, :, cut(q)], 0.0)
            out[:, 0, cut(q)] = result

    with jax.named_scope("drain"):
        for make, when in sent:
            if when is None:
                make().wait_send()
            else:
                @pl.when(when)
                def _(make=make):
                    make().wait_send()
        for i in range(chunks):
            for off in others:
                sum_copy(i, off).wait_send()


def per_device(bands, grids, orbitals):
    blocks, rows, cells = orbitals.shape
    length = rows * grids
    assert blocks == 1 and bands == 2 * grids and length * length == cells
    assert 2 * length <= 128
    basis = real_basis(length)
    consts = np.zeros((2, 256 + 2 * length, 256))
    for n, table in enumerate((basis, basis.T)):
        high = table.astype(np.float32).astype(BF16).astype(np.float64)
        for m, part in enumerate((high, table - high)):
            for k in range(4):
                r = 128 * (k // 2) + (k % 2) * length
                s = 128 * m + (k % 2) * length
                consts[n, r:r + length, s:s + length] = part
            for k in range(2):
                consts[n, 256 + m * length:256 + (m + 1) * length, k * length:(k + 1) * length] = part.T
    consts = jnp.asarray(consts.astype(BF16))
    slab = (rows, cells)
    dma = lambda *n: pltpu.SemaphoreType.DMA(n)
    vmem = lambda *shape: pltpu.VMEM(shape, F32)
    pairs = bands // 2
    pieces = 3
    chunks = length // 8
    result = pl.pallas_call(
        functools.partial(kernel, bands, grids, length, pieces),
        out_shape=jax.ShapeDtypeStruct((rows, 1, cells), F32),
        in_specs=[pl.BlockSpec(memory_space=pltpu.HBM)] * 2,
        out_specs=pl.BlockSpec(memory_space=pltpu.VMEM),
        scratch_shapes=[
            vmem(bands, *slab), vmem(3, grids, *slab),
            vmem(grids, *slab), vmem(grids, *slab), vmem(bands, *slab),
            vmem(grids, bands, 128), vmem(bands, bands, 128),
            vmem(length, cells), vmem(2, length, cells),
            vmem(length * length, 128), vmem(length, length, 128),
            vmem(length, 8 * length), pltpu.VMEM(consts.shape, BF16),
            dma(rows), dma(rows), pltpu.SemaphoreType.DMA,
            dma(2 * reach, pieces), dma(bands, pieces), dma(2 * pairs, pieces), dma(bands), dma(bands),
            dma(grids, pieces), dma(grids, pieces), dma(pairs, pieces), dma(grids, pieces),
            dma(grids, pieces), dma(grids, pieces),
            dma(grids, chunks), dma(grids, chunks),
            dma(reach + 1, pieces), dma(bands, pieces), dma(pairs, pieces), dma(pairs, pieces),
            dma(grids), dma(grids), dma(bands), dma(bands),
        ],
        compiler_params=pltpu.CompilerParams(
            collective_id=0, has_side_effects=True, vmem_limit_bytes=40 * 1024 * 1024
        ),
    )(orbitals.reshape(rows, 1, cells), consts)
    return result.reshape(orbitals.shape)


def solution(mesh):
    bands, grids = mesh.shape["band"], mesh.shape["grid"]
    return jax.shard_map(
        functools.partial(per_device, bands, grids), mesh=mesh,
        in_specs=(P("band", "grid", None),), out_specs=P("band", "grid", None), check_vma=False,
    )
```

```python
import functools
import math

import jax
import jax.numpy as jnp
import numpy as np
from jax import lax
from jax.experimental import pallas as pl
from jax.experimental.pallas import tpu as pltpu
from jax.sharding import PartitionSpec as P

MESH = pl.DeviceIdType.MESH
F32 = jnp.float32
BF16 = jnp.bfloat16
coulomb_scale = 50.0
reach = 2


def real_basis(length):
    n = np.arange(length)[:, None]
    m = np.arange(length)[None, :]
    angle = 2.0 * math.pi * ((n * np.minimum(m, length - m)) % length) / length
    table = np.where(m <= length // 2, np.cos(angle), np.sin(angle))
    weight = np.where((m == 0) | (2 * m == length), 1.0, 2.0)
    return table * np.sqrt(weight / length)


def split(value):
    high = value.astype(BF16)
    return high, (value - high.astype(F32)).astype(BF16)


def right(value, table):
    both = jnp.concatenate(split(value), axis=1)
    out = jnp.dot(both, table, preferred_element_type=F32)
    half = out.shape[1] // 2
    return out[:, :half] + out[:, half:]


def left(table, value):
    both = jnp.concatenate(split(value), axis=0)
    out = jnp.dot(table, both, preferred_element_type=F32)
    half = out.shape[0] // 2
    return out[:half] + out[half:]


def kernel(
    bands, grids, length, pieces,
    phi, consts, out,
    slabs, cubes, field, sums, exs, proj_grid, proj_band,
    dense_own, dense_part, work, coulomb, dense_field, tables,
    phi_sem, own_sem, consts_sem, slab_send, slab_recv, relay_send, fwd_send, fwd_recv,
    own_send, own_recv, part_send, part_recv, pfwd_send, pfwd_recv,
    sum_send, sum_recv, ex_send, ex_recv, xrelay_send, xfwd_send,
    pg_send, pg_recv, pb_send, pb_recv,
):
    b = lax.axis_index("band")
    g = lax.axis_index("grid")
    p = b // 2
    c = b % 2
    sibling = p * 2 + (1 - c)
    rows = length // grids
    pairs = bands // 2
    step = 8
    chunk = step * length
    chunks = length // step
    width = length * length // pieces
    per_piece = chunks // pieces
    others = range(1, grids)

    def remote(src, dst, send, recv, band, grid):
        return pltpu.make_async_remote_copy(
            src_ref=src, dst_ref=dst, send_sem=send, recv_sem=recv,
            device_id=(band, grid), device_id_type=MESH,
        )

    def cut(q):
        return pl.ds(q * width, width)

    def on_line(layer):
        return (layer >= 0) & (layer < pairs)

    sent = []

    def go(make, when=None):
        if when is None:
            make().start()
        else:
            @pl.when(when)
            def _():
                make().start()
        sent.append((make, when))

    def peer(off):
        return lax.rem(g + off, grids)

    barrier = pltpu.get_barrier_semaphore()
    expected = 1 + grids - 1
    pl.semaphore_signal(barrier, inc=1, device_id=(sibling, g), device_id_type=MESH)
    for off in others:
        pl.semaphore_signal(barrier, inc=1, device_id=(b, peer(off)), device_id_type=MESH)
    for d in range(1, min(reach, pairs - 1) + 1):
        for sign in (1, -1):
            layer = p + sign * d

            @pl.when(on_line(layer))
            def _(layer=layer):
                pl.semaphore_signal(barrier, inc=1, device_id=(layer * 2 + c, g), device_id_type=MESH)

            expected = expected + on_line(layer).astype(jnp.int32)

    local = []
    for x in range(rows):
        local.append(pltpu.make_async_copy(phi.at[x], slabs.at[b, pl.ds(x, 1), :], phi_sem.at[x]))
    for x in range(rows):
        local.append(pltpu.make_async_copy(phi.at[x], cubes.at[0, g, pl.ds(x, 1), :], own_sem.at[x]))
    local.append(pltpu.make_async_copy(consts, tables, consts_sem))
    for copy in local:
        copy.start()

    def freq_of(m):
        f = jnp.minimum(m, length - m).astype(F32)
        return f * f

    def freq(shape, dim, base):
        return freq_of(lax.broadcasted_iota(jnp.int32, shape, dim) + base)

    def coulomb_step(i, carry):
        shape = (step, length, 128)
        lane = lax.broadcasted_iota(jnp.int32, shape, 2)
        lane = jnp.where(lane < length, lane, lane - length)
        squared = freq(shape, 0, i * step) + freq(shape, 1, 0) + freq_of(lane)
        coulomb[pl.ds(i * step, step)] = jnp.where(
            squared > 0.0, coulomb_scale / jnp.maximum(squared, 1.0), 0.0
        )
        return carry

    with jax.named_scope("coul"):
        lax.fori_loop(0, chunks, coulomb_step, 0)
        for copy in local:
            copy.wait()
    with jax.named_scope("barr"):
        pl.semaphore_wait(barrier, expected)

    def slab_copy(src_band, layer, q, send):
        here = slabs.at[src_band, :, cut(q)]
        return remote(here, here, send, slab_recv.at[src_band, q], layer * 2 + c, g)

    def sibling_part(s, q, src):
        return remote(src, cubes.at[1 + c, s, :, cut(q)], pfwd_send.at[s, q], pfwd_recv.at[s, q], sibling, g)

    for q in range(pieces):
        for d in range(min(reach, pairs - 1), 0, -1):
            for sign in (1, -1):
                layer = p + sign * d
                index = 2 * (d - 1) + (sign < 0)
                go(lambda layer=layer, index=index, q=q: slab_copy(b, layer, q, slab_send.at[index, q]),
                   on_line(layer))
        for off in others:
            go(lambda off=off, q=q: remote(
                slabs.at[b, :, cut(q)], cubes.at[0, g, :, cut(q)],
                own_send.at[off, q], own_recv.at[g, q], b, peer(off)))
        go(lambda q=q: sibling_part(g, q, slabs.at[b, :, cut(q)]), g == p)

    def partner_copy(layer, q):
        return remote(
            slabs.at[layer * 2 + c, :, cut(q)], cubes.at[1 + c, g, :, cut(q)],
            part_send.at[layer, q], part_recv.at[g, q], b, layer,
        )

    def take_slab(sign, d, q):
        layer = p - sign * d
        band = layer * 2 + c
        there = on_line(layer)

        @pl.when(there)
        def _():
            slab_copy(band, p, q, slab_send.at[0, q]).wait_recv()

        if d >= reach:
            way = 2 * d + (sign < 0)
            go(lambda: slab_copy(band, p + sign, q, relay_send.at[way, q]), there & on_line(p + sign))
        go(lambda: partner_copy(layer, q), there & (layer != g))
        go(lambda: sibling_part(g, q, slabs.at[band, :, cut(q)]), there & (layer == g))

    def take_part(off, q):
        other = peer(off)
        mine = cubes.at[0, other, :, cut(q)]
        remote(mine, mine, own_send.at[0, q], own_recv.at[other, q], b, other).wait_recv()
        slot = jnp.where(g == p, 0, 1 + c)

        @pl.when(g != p)
        def _():
            here = cubes.at[1 + c, other, :, cut(q)]
            remote(here, here, part_send.at[0, q], part_recv.at[other, q], b, other).wait_recv()

        go(lambda: sibling_part(other, q, cubes.at[slot, other, :, cut(q)]))

    def collect(q):
        for s in range(grids):
            here = cubes.at[2 - c, s, :, cut(q)]
            remote(here, here, pfwd_send.at[0, q], pfwd_recv.at[s, q], sibling, g).wait_recv()
        slot = jnp.where(g == p, 0, 1 + c)
        for s in range(grids):
            here = slice(s * rows, (s + 1) * rows)
            dense_own[here, cut(q)] = cubes[0, s, :, cut(q)]
            dense_part[1 - c, here, cut(q)] = cubes[2 - c, s, :, cut(q)]

            @pl.when(s != g)
            def _(s=s, here=here):
                dense_part[c, here, cut(q)] = cubes[slot, s, :, cut(q)]

            @pl.when(s == g)
            def _(s=s, here=here):
                dense_part[c, here, cut(q)] = slabs[2 * g + c, :, cut(q)]

    padding = jnp.zeros((128 - 2 * length, chunk), F32)

    def wide(n):
        return tables[n, 0:256, :]

    def tall(n):
        return tables[n, 256:256 + 2 * length, 0:2 * length]

    def rows_of(m):
        return pl.ds(pl.multiple_of(m * length, 8), length)

    def lanes_of(i):
        return pl.ds(pl.multiple_of(i * chunk, 128), chunk)

    def stage_in(i, carry):
        lanes = lanes_of(i)
        mine = dense_own[:, lanes]
        density = [mine * dense_part[k, :, lanes] for k in range(2)]
        value = right(jnp.concatenate(density + [padding], axis=0).T, wide(0))
        for s in range(0, step, 2):
            two = jnp.concatenate([value[n * length:(n + 1) * length] for n in (s, s + 1)], axis=1)
            two = left(tall(0), two)
            for n in range(2):
                work[rows_of(i * step + s + n), :] = two[:, n * 128:(n + 1) * 128]
        return carry

    def stage_mid(i, carry):
        for s in range(0, step, 2):
            here = [pl.ds(i * step + s + n, length, length) for n in range(2)]
            two = left(tall(0), jnp.concatenate([work[h, :] for h in here], axis=1))
            two = two * jnp.concatenate([coulomb[i * step + s + n] for n in range(2)], axis=1)
            two = left(tall(1), two)
            for n in range(2):
                work[here[n], :] = two[:, n * 128:(n + 1) * 128]
        return carry

    def sum_copy(i, off):
        lanes = lanes_of(i)
        other = peer(off)
        return remote(field.at[other, :, lanes], sums.at[g, :, lanes],
                      sum_send.at[off, i], sum_recv.at[g, i], b, other)

    def send_sums(i):
        for off in others:
            sum_copy(i, off).start()

    def stage_out(i, carry):
        lanes = lanes_of(i)
        value = []
        for s in range(0, step, 2):
            two = jnp.concatenate([work[rows_of(i * step + s + n), :] for n in range(2)], axis=1)
            two = left(tall(1), two)
            value += [two[:, n * 128:(n + 1) * 128] for n in range(2)]
        value = right(jnp.concatenate(value, axis=0), wide(1)).T
        dense_field[...] = sum(
            dense_part[k, :, lanes] * value[k * length:(k + 1) * length] for k in range(2)
        )
        for s in range(grids):
            field[s, :, lanes] = dense_field[s * rows:(s + 1) * rows, :]

        @pl.when(i > 0)
        def _():
            send_sums(i - 1)

        return carry

    columns = [None] * bands

    def ex_copy(src_band, band, q, send):
        here = exs.at[src_band, :, cut(q)]
        return remote(here, here, send, ex_recv.at[src_band, q], band, g)

    def exchange_piece(q):
        for i in range(q * per_piece, (q + 1) * per_piece):
            lanes = pl.ds(i * chunk, chunk)
            for off in others:
                other = peer(off)
                here = sums.at[other, :, lanes]
                remote(here, here, sum_send.at[0, i], sum_recv.at[other, i], b, other).wait_recv()
        value = field[g, :, cut(q)]
        for off in others:
            value = value + sums[peer(off), :, cut(q)]
        value = -value
        exs[b, :, cut(q)] = value
        for d in range(min(reach, pairs - 1), 0, -1):
            go(lambda d=d: ex_copy(b, (p + d) * 2 + c, q, ex_send.at[d, q]), on_line(p + d))
        go(lambda: ex_copy(b, sibling, q, ex_send.at[0, q]), c == 0)
        for k in range(bands):
            product = jnp.sum(slabs[k, :, cut(q)] * value, axis=0, keepdims=True)
            product = sum(product[:, n:n + 128] for n in range(0, width, 128))
            columns[k] = product if columns[k] is None else columns[k] + product

    near = range(1, min(reach, pairs - 1) + 1)
    far = range(reach + 1, pairs)
    with jax.named_scope("slabnear"):
        for q in range(pieces):
            for d in near:
                for sign in (1, -1):
                    take_slab(sign, d, q)
    with jax.named_scope("slabfar"):
        for d in far:
            for q in range(pieces):
                for sign in (1, -1):
                    take_slab(sign, d, q)
    for q in range(pieces):
        with jax.named_scope(f"part{q}"):
            for off in others:
                take_part(off, q)
        if q >= 1:
            with jax.named_scope(f"collect{q-1}"):
                collect(q - 1)
            with jax.named_scope(f"stagein{q-1}"):
                lax.fori_loop((q - 1) * per_piece, q * per_piece, stage_in, 0, unroll=True)
    with jax.named_scope("collectlast"):
        collect(pieces - 1)
    with jax.named_scope("stageinlast"):
        lax.fori_loop((pieces - 1) * per_piece, chunks, stage_in, 0, unroll=True)

    def whole_slab(band):
        here = slabs.at[band]
        return remote(here, here, fwd_send.at[band], fwd_recv.at[band], sibling, g)

    for s in range(pairs):
        go(lambda s=s: whole_slab(2 * s + c))
    with jax.named_scope("mid"):
        lax.fori_loop(0, chunks, stage_mid, 0, unroll=True)
    with jax.named_scope("out"):
        for q in range(pieces):
            lax.fori_loop(q * per_piece, (q + 1) * per_piece, stage_out, 0, unroll=True)
        send_sums(chunks - 1)
        for s in range(pairs):
            whole_slab(2 * s + 1 - c).wait_recv()
    for q in range(pieces):
        with jax.named_scope(f"exch{q}"):
            exchange_piece(q)

    total = jnp.sum(jnp.concatenate(columns, axis=0), axis=1, keepdims=True)
    proj_grid[g] = jnp.broadcast_to(total, (bands, 128))
    for off in others:
        go(lambda off=off: remote(proj_grid.at[g], proj_grid.at[g], pg_send.at[off], pg_recv.at[g], b, peer(off)))

    def take_exchange(d, q):
        layer = p - d
        band = layer * 2 + c
        there = layer >= 0

        @pl.when(there)
        def _():
            ex_copy(band, b, q, ex_send.at[0, q]).wait_recv()

        if d >= reach:
            go(lambda: ex_copy(band, (p + 1) * 2 + c, q, xrelay_send.at[d, q]), there & on_line(p + 1))
        go(lambda: ex_copy(band, sibling, q, xfwd_send.at[d, q]), there)

    with jax.named_scope("pex0"):
        for d in near:
            take_exchange(d, 0)
    with jax.named_scope("projgrid"):
        for off in others:
            other = peer(off)
            here = proj_grid.at[other]
            remote(here, here, pg_send.at[0], pg_recv.at[other], b, other).wait_recv()
        total = proj_grid[0]
        for s in range(1, grids):
            total = total + proj_grid[s]
        proj_band[b] = total
    for off in range(1, bands):
        go(lambda off=off: remote(
            proj_band.at[b], proj_band.at[b], pb_send.at[off], pb_recv.at[b], b + off, g), b + off < bands)
    with jax.named_scope("pexnear"):
        for q in range(1, pieces):
            for d in near:
                take_exchange(d, q)
    with jax.named_scope("pexfar"):
        for d in far:
            for q in range(pieces):
                take_exchange(d, q)
    with jax.named_scope("projband"):
        for l in range(bands - 1):
            @pl.when(l < b)
            def _(l=l):
                here = proj_band.at[l]
                remote(here, here, pb_send.at[0], pb_recv.at[l], l, g).wait_recv()

    row = lax.broadcasted_iota(jnp.int32, (bands, 128), 0)
    col = lax.broadcasted_iota(jnp.int32, (bands, 128), 1)
    matrix = jnp.zeros((bands, 128), F32)
    mirrored = jnp.zeros((bands, 128), F32)
    for l in range(bands):
        entries = proj_band[l]
        matrix = jnp.where(col == l, entries, matrix)
        flipped = jnp.sum(jnp.where(row == col, entries, 0.0), axis=0, keepdims=True)
        mirrored = jnp.where(row == l, flipped, mirrored)
    definite = (matrix + mirrored) * (-0.5 / float(length**3))
    unit = (col == row) | (col == row + bands)
    definite = jnp.where((row <= b) & (col <= b), definite, jnp.where(unit, 1.0, 0.0))
    for j in range(bands - 1):
        line = definite[j:j + 1, :]
        ratio = definite[:, j:j + 1] / definite[j:j + 1, j:j + 1]
        definite = definite - jnp.where(row > j, ratio * line, 0.0)
    pick = jnp.sum(jnp.where(row == b, definite, 0.0), axis=0, keepdims=True)
    pivot = jnp.sum(jnp.where(col[0:1] == b, pick, 0.0), axis=1, keepdims=True)
    pick = pick / jnp.sqrt(pivot)

    with jax.named_scope("final"):
        for q in range(pieces):
            for d in range(pairs):
                layer = p - d

                @pl.when((layer >= 0) if d > 0 else (c == 1))
                def _(layer=layer):
                    ex_copy(layer * 2 + 1 - c, b, q, ex_send.at[0, q]).wait_recv()

            result = jnp.zeros((rows, width), F32)
            for l in range(bands):
                result = result + pick[:, bands + l:bands + l + 1] * jnp.where(l <= b, exs[l, :, cut(q)], 0.0)
            out[:, 0, cut(q)] = result

    with jax.named_scope("drain"):
        for make, when in sent:
            if when is None:
                make().wait_send()
            else:
                @pl.when(when)
                def _(make=make):
                    make().wait_send()
        for i in range(chunks):
            for off in others:
                sum_copy(i, off).wait_send()


def per_device(bands, grids, orbitals):
    blocks, rows, cells = orbitals.shape
    length = rows * grids
    assert blocks == 1 and bands == 2 * grids and length * length == cells
    assert 2 * length <= 128
    basis = real_basis(length)
    consts = np.zeros((2, 256 + 2 * length, 256))
    for n, table in enumerate((basis, basis.T)):
        high = table.astype(np.float32).astype(BF16).astype(np.float64)
        for m, part in enumerate((high, table - high)):
            for k in range(4):
                r = 128 * (k // 2) + (k % 2) * length
                s = 128 * m + (k % 2) * length
                consts[n, r:r + length, s:s + length] = part
            for k in range(2):
                consts[n, 256 + m * length:256 + (m + 1) * length, k * length:(k + 1) * length] = part.T
    consts = jnp.asarray(consts.astype(BF16))
    slab = (rows, cells)
    dma = lambda *n: pltpu.SemaphoreType.DMA(n)
    vmem = lambda *shape: pltpu.VMEM(shape, F32)
    pairs = bands // 2
    pieces = 3
    chunks = length // 8
    result = pl.pallas_call(
        functools.partial(kernel, bands, grids, length, pieces),
        out_shape=jax.ShapeDtypeStruct((rows, 1, cells), F32),
        in_specs=[pl.BlockSpec(memory_space=pltpu.HBM)] * 2,
        out_specs=pl.BlockSpec(memory_space=pltpu.VMEM),
        scratch_shapes=[
            vmem(bands, *slab), vmem(3, grids, *slab),
            vmem(grids, *slab), vmem(grids, *slab), vmem(bands, *slab),
            vmem(grids, bands, 128), vmem(bands, bands, 128),
            vmem(length, cells), vmem(2, length, cells),
            vmem(length * length, 128), vmem(length, length, 128),
            vmem(length, 8 * length), pltpu.VMEM(consts.shape, BF16),
            dma(rows), dma(rows), pltpu.SemaphoreType.DMA,
            dma(2 * reach, pieces), dma(bands, pieces), dma(2 * pairs, pieces), dma(bands), dma(bands),
            dma(grids, pieces), dma(grids, pieces), dma(pairs, pieces), dma(grids, pieces),
            dma(grids, pieces), dma(grids, pieces),
            dma(grids, chunks), dma(grids, chunks),
            dma(reach + 1, pieces), dma(bands, pieces), dma(pairs, pieces), dma(pairs, pieces),
            dma(grids), dma(grids), dma(bands), dma(bands),
        ],
        compiler_params=pltpu.CompilerParams(
            collective_id=0, has_side_effects=True, vmem_limit_bytes=40 * 1024 * 1024
        ),
    )(*(pltpu.with_memory_space_constraint(a, pltpu.HBM) for a in (orbitals.reshape(rows, 1, cells), consts)))
    return result.reshape(orbitals.shape)


def solution(mesh):
    bands, grids = mesh.shape["band"], mesh.shape["grid"]
    return jax.shard_map(
        functools.partial(per_device, bands, grids), mesh=mesh,
        in_specs=(P("band", "grid", None),), out_specs=P("band", "grid", None), check_vma=False,
    )
```
